32 devices in a mesh: t: 4 (over z), v: 8 (over y, x, core).
Axes of the slice: x: 2, y: 2, z: 4, core: 2. Of those that a mesh axis runs over, the one named last changes fastest.
Arguments:
- hidden_in: bfloat16 [1024, 2304], replicated
- seq_lens: int32 [1024], replicated
- target: int32 [1024], replicated
- g_attn_pre: bfloat16 [2304], replicated
- w_q: bfloat16 [2304, 2048], P(None, 't')
- w_k: bfloat16 [2304, 1024], P(None, 't')
- w_v: bfloat16 [2304, 1024], P(None, 't')
- w_o: bfloat16 [2048, 2304], P('t')
- g_attn_post: bfloat16 [2304], replicated
- g_mlp_pre: bfloat16 [2304], replicated
- w_gate: bfloat16 [2304, 9216], P(None, 't')
- w_up: bfloat16 [2304, 9216], P(None, 't')
- w_down: bfloat16 [9216, 2304], P('t')
- g_mlp_post: bfloat16 [2304], replicated
- g_final: bfloat16 [2304], replicated
- k_cache: bfloat16 [1024, 32, 4, 256], P(None, None, 't')
- v_cache: bfloat16 [1024, 32, 4, 256], P(None, None, 't')
- embed_table: bfloat16 [256000, 2304], P(('v', 't'))
Outputs:
- output 1: float32 [1024], replicated
- output 2: bfloat16 [1024, 2304], replicated
All inputs are finite; a program needn't handle non-finite values.
Results may differ from the reference program's by a relative error of at most 0.0078882.
Values sent between devices are 32-bit elements.
A program may use at most 1 GiB of HBM per device.

```python
import jax
import jax.numpy as jnp
from jax import lax

D = 2304
HEADS = 8
KV_HEADS = 4
HEAD = 256
FF = 9216
VOCAB = 256000
TOKENS = 1024
CTX = 32

ATTN_CAP = 50.0
FINAL_CAP = 30.0
NORM_EPS = 1e-6
ROPE_BASE = 10000.0


def rms_norm(values, gain_vec):
    x_f32 = values.astype(jnp.float32)
    scaled = x_f32 * lax.rsqrt(jnp.mean(x_f32 * x_f32, axis=-1, keepdims=True) + NORM_EPS)
    return scaled * (1.0 + gain_vec.astype(jnp.float32))


def rotary(values, positions):
    half_dim = values.shape[-1] // 2
    inv_freq = ROPE_BASE ** (-2.0 * jnp.arange(half_dim, dtype=jnp.float32) / values.shape[-1])
    angles = positions.astype(jnp.float32)[:, None] * inv_freq[None, :]
    angles = angles.reshape((values.shape[0],) + (1,) * (values.ndim - 2) + (half_dim,))
    cos_t = jnp.cos(angles)
    sin_t = jnp.sin(angles)
    x_low = values[..., :half_dim]
    x_high = values[..., half_dim:]
    return jnp.concatenate([x_low * cos_t - x_high * sin_t, x_high * cos_t + x_low * sin_t], axis=-1)


def setup_inputs(seed: int = 0) -> dict:
    keys = jax.random.split(jax.random.key(seed), 20)

    def normal_draw(sub_key, dims, scale_by):
        return (jax.random.normal(sub_key, dims, jnp.float32) * scale_by).astype(jnp.bfloat16)

    int_keys = jax.random.split(keys[19], 4)
    token_ids = jnp.arange(TOKENS)
    seq_lens = jax.random.randint(int_keys[0], (TOKENS,), 1, CTX + 1)
    picked = jax.random.permutation(int_keys[1], TOKENS)
    seq_lens = jnp.where(token_ids == picked[0], CTX, seq_lens)
    seq_lens = jnp.where(token_ids == picked[1], 1, seq_lens).astype(jnp.int32)
    stride = VOCAB // TOKENS
    target = token_ids * stride + jax.random.randint(int_keys[2], (TOKENS,), 0, stride)
    target = jax.random.permutation(int_keys[3], target).astype(jnp.int32)
    d_scale = D ** -0.5
    return {
        'hidden_in': normal_draw(keys[0], (TOKENS, D), 1.0),
        'seq_lens': seq_lens,
        'target': target,
        'g_attn_pre': normal_draw(keys[1], (D,), 0.4),
        'w_q': normal_draw(keys[2], (D, HEADS * HEAD), 4.0 * d_scale),
        'w_k': normal_draw(keys[3], (D, KV_HEADS * HEAD), 4.0 * d_scale),
        'w_v': normal_draw(keys[4], (D, KV_HEADS * HEAD), d_scale),
        'w_o': normal_draw(keys[5], (HEADS * HEAD, D), (HEADS * HEAD) ** -0.5),
        'g_attn_post': normal_draw(keys[6], (D,), 0.4),
        'g_mlp_pre': normal_draw(keys[7], (D,), 0.4),
        'w_gate': normal_draw(keys[8], (D, FF), d_scale),
        'w_up': normal_draw(keys[9], (D, FF), d_scale),
        'w_down': normal_draw(keys[10], (FF, D), FF ** -0.5),
        'g_mlp_post': normal_draw(keys[11], (D,), 0.4),
        'g_final': normal_draw(keys[12], (D,), 0.4),
        'k_cache': normal_draw(keys[13], (TOKENS, CTX, KV_HEADS, HEAD), 4.0),
        'v_cache': normal_draw(keys[14], (TOKENS, CTX, KV_HEADS, HEAD), 1.0),
        'embed_table': normal_draw(keys[15], (VOCAB, D), 25.0 * d_scale),
    }


def reference(hidden_in, seq_lens, target, g_attn_pre, w_q, w_k, w_v, w_o, g_attn_post, g_mlp_pre, w_gate, w_up, w_down, g_mlp_post, g_final, k_cache, v_cache, embed_table):
    group_size = HEADS // KV_HEADS
    score_scale = HEAD ** -0.5
    normed = rms_norm(hidden_in, g_attn_pre).astype(jnp.bfloat16)
    q_rot = rotary(jnp.dot(normed, w_q, preferred_element_type=jnp.float32).reshape(TOKENS, KV_HEADS, group_size, HEAD), seq_lens).astype(jnp.bfloat16)
    k_rot = rotary(jnp.dot(normed, w_k, preferred_element_type=jnp.float32).reshape(TOKENS, KV_HEADS, HEAD), seq_lens).astype(jnp.bfloat16)
    v_new = jnp.dot(normed, w_v, preferred_element_type=jnp.float32).astype(jnp.bfloat16).reshape(TOKENS, KV_HEADS, HEAD)

    def attend(operands):
        q_tok, k_tok, v_tok, keys_tok, vals_tok, len_tok = operands
        q_f32 = q_tok.astype(jnp.float32)
        s_cache = jnp.einsum('kgd,tkd->kgt', q_f32, keys_tok.astype(jnp.float32)) * score_scale
        s_new = jnp.einsum('kgd,kd->kg', q_f32, k_tok.astype(jnp.float32)) * score_scale
        s_cache = ATTN_CAP * jnp.tanh(s_cache / ATTN_CAP)
        s_new = ATTN_CAP * jnp.tanh(s_new / ATTN_CAP)
        s_cache = jnp.where(jnp.arange(CTX) < len_tok, s_cache, -1e30)
        row_max = jnp.maximum(jnp.max(s_cache, axis=-1), s_new)
        p_cache = jnp.exp(s_cache - row_max[..., None])
        p_new = jnp.exp(s_new - row_max)
        denominator = jnp.sum(p_cache, axis=-1) + p_new
        weighted = jnp.einsum('kgt,tkd->kgd', p_cache.astype(jnp.bfloat16).astype(jnp.float32), vals_tok.astype(jnp.float32))
        weighted = weighted + p_new.astype(jnp.bfloat16).astype(jnp.float32)[..., None] * v_tok.astype(jnp.float32)[:, None, :]
        return (weighted / denominator[..., None]).astype(jnp.bfloat16)

    attn_vec = lax.map(attend, (q_rot, k_rot, v_new, k_cache, v_cache, seq_lens))
    attn_out = jnp.dot(attn_vec.reshape(TOKENS, HEADS * HEAD), w_o, preferred_element_type=jnp.float32)
    hidden_mid = (hidden_in.astype(jnp.float32) + rms_norm(attn_out, g_attn_post)).astype(jnp.bfloat16)
    mlp_in = rms_norm(hidden_mid, g_mlp_pre).astype(jnp.bfloat16)
    gate_proj = jnp.dot(mlp_in, w_gate, preferred_element_type=jnp.float32)
    up_proj = jnp.dot(mlp_in, w_up, preferred_element_type=jnp.float32)
    activated = (jax.nn.gelu(gate_proj, approximate=True) * up_proj).astype(jnp.bfloat16)
    mlp_out = jnp.dot(activated, w_down, preferred_element_type=jnp.float32)
    hidden_out = (hidden_mid.astype(jnp.float32) + rms_norm(mlp_out, g_mlp_post)).astype(jnp.bfloat16)
    final_h = rms_norm(hidden_out, g_final).astype(jnp.bfloat16)

    blocks = 16
    block_rows = VOCAB // blocks
    table_blocks = embed_table.reshape(blocks, block_rows, D)
    starts = jnp.arange(blocks) * block_rows

    def block_stats(operands):
        table_block, start_row = operands
        logits = jnp.dot(final_h, table_block.T, preferred_element_type=jnp.float32)
        capped = FINAL_CAP * jnp.tanh(logits / FINAL_CAP)
        block_max = jnp.max(capped, axis=1)
        block_sum = jnp.sum(jnp.exp(capped - block_max[:, None]), axis=1)
        hit_mask = (start_row + jnp.arange(block_rows))[None, :] == target[:, None]
        block_tgt = jnp.sum(jnp.where(hit_mask, capped, 0.0), axis=1)
        return block_max, block_sum, block_tgt

    all_max, all_sum, all_tgt = lax.map(block_stats, (table_blocks, starts))
    glob_max = jnp.max(all_max, axis=0)
    log_norm = glob_max + jnp.log(jnp.sum(all_sum * jnp.exp(all_max - glob_max[None, :]), axis=0))
    logprob = jnp.sum(all_tgt, axis=0) - log_norm
    return logprob, hidden_out
```

```python
import functools
import math

import jax
import jax.numpy as jnp
from jax import lax
from jax.experimental import pallas as pl
from jax.experimental.pallas import tpu as pltpu
from jax.sharding import PartitionSpec as P

ATTN_CAP = 50.0
FINAL_CAP = 30.0
NORM_EPS = 1e-6
ROPE_BASE = 10000.0
MESH = pl.DeviceIdType.MESH
VMEM_LIMIT = 66_000_000


def rms_norm(values, gain_vec):
    x_f32 = values.astype(jnp.float32)
    scaled = x_f32 * lax.rsqrt(jnp.mean(x_f32 * x_f32, axis=-1, keepdims=True) + NORM_EPS)
    return scaled * (1.0 + gain_vec.astype(jnp.float32))


def rotary(values, positions):
    half_dim = values.shape[-1] // 2
    inv_freq = ROPE_BASE ** (-2.0 * jnp.arange(half_dim, dtype=jnp.float32) / values.shape[-1])
    angles = positions.astype(jnp.float32)[:, None] * inv_freq[None, :]
    angles = angles.reshape((values.shape[0],) + (1,) * (values.ndim - 2) + (half_dim,))
    cos_t = jnp.cos(angles)
    sin_t = jnp.sin(angles)
    x_low = values[..., :half_dim]
    x_high = values[..., half_dim:]
    return jnp.concatenate([x_low * cos_t - x_high * sin_t, x_high * cos_t + x_low * sin_t], axis=-1)


def attention(normed, seq_lens, w_q, w_k, w_v, k_cache, v_cache):
    tokens, ctx_len, kv_heads, head_dim = k_cache.shape
    group_size = w_q.shape[1] // (kv_heads * head_dim)
    score_scale = head_dim ** -0.5
    q_rot = rotary(jnp.dot(normed, w_q, preferred_element_type=jnp.float32).reshape(tokens, kv_heads, group_size, head_dim), seq_lens).astype(jnp.bfloat16)
    k_rot = rotary(jnp.dot(normed, w_k, preferred_element_type=jnp.float32).reshape(tokens, kv_heads, head_dim), seq_lens).astype(jnp.bfloat16)
    v_new = jnp.dot(normed, w_v, preferred_element_type=jnp.float32).astype(jnp.bfloat16).reshape(tokens, kv_heads, head_dim)
    s_cache = jnp.einsum('nkgd,ntkd->nkgt', q_rot, k_cache, preferred_element_type=jnp.float32) * score_scale
    s_new = jnp.einsum('nkgd,nkd->nkg', q_rot, k_rot, preferred_element_type=jnp.float32) * score_scale
    s_cache = ATTN_CAP * jnp.tanh(s_cache / ATTN_CAP)
    s_new = ATTN_CAP * jnp.tanh(s_new / ATTN_CAP)
    valid_mask = jnp.arange(ctx_len)[None, :] < seq_lens[:, None]
    s_cache = jnp.where(valid_mask[:, None, None, :], s_cache, -1e30)
    row_max = jnp.maximum(jnp.max(s_cache, axis=-1), s_new)
    p_cache = jnp.exp(s_cache - row_max[..., None])
    p_new = jnp.exp(s_new - row_max)
    denominator = jnp.sum(p_cache, axis=-1) + p_new
    weighted = jnp.einsum('nkgt,ntkd->nkgd', p_cache.astype(jnp.bfloat16), v_cache, preferred_element_type=jnp.float32)
    weighted = weighted + p_new.astype(jnp.bfloat16).astype(jnp.float32)[..., None] * v_new.astype(jnp.float32)[:, :, None, :]
    return (weighted / denominator[..., None]).astype(jnp.bfloat16).reshape(tokens, kv_heads * group_size * head_dim)


def line_reduce_kernel(chunks, lag, part_ref, res_ref, gain_ref, out_ref, sum_buf, end_buf, mate_buf, res_buf, send_sem, recv_sem):
    t = lax.axis_index('t')
    rows = part_ref.shape[0] // chunks
    is_end = t * (3 - t) == 0
    inner = 1 + t // 3
    outer = 3 * (t - 1)
    mate = 3 - t
    barrier = pltpu.get_barrier_semaphore()

    def piece(ref, c):
        return ref.at[pl.ds(c * rows, rows)]

    def copy(src, dst, stage, c, to):
        return pltpu.make_async_remote_copy(
            src_ref=piece(src, c), dst_ref=piece(dst, c), send_sem=send_sem.at[stage, c],
            recv_sem=recv_sem.at[stage, c], device_id={'t': to}, device_id_type=MESH)

    @pl.when(is_end)
    def _():
        pl.semaphore_signal(barrier, inc=1, device_id={'t': inner}, device_id_type=MESH)
        pl.semaphore_wait(barrier, 1)
        for c in range(chunks):
            copy(part_ref, end_buf, 0, c, inner).start()
        for c in range(chunks):
            copy(res_buf, res_buf, 2, c, inner).wait_recv()
            piece(out_ref, c)[...] = piece(res_buf, c)[...].astype(out_ref.dtype)
        for c in range(chunks):
            copy(part_ref, end_buf, 0, c, inner).wait_send()

    @pl.when(jnp.logical_not(is_end))
    def _():
        pl.semaphore_signal(barrier, inc=1, device_id={'t': outer}, device_id_type=MESH)
        pl.semaphore_signal(barrier, inc=1, device_id={'t': mate}, device_id_type=MESH)
        pl.semaphore_wait(barrier, 2)
        for i in range(chunks + lag):
            if i < chunks:
                copy(part_ref, end_buf, 0, i, outer).wait_recv()
                piece(sum_buf, i)[...] = piece(part_ref, i)[...] + piece(end_buf, i)[...]
                copy(sum_buf, mate_buf, 1, i, mate).start()
            j = i - lag
            if j >= 0:
                copy(sum_buf, mate_buf, 1, j, mate).wait_recv()
                total = piece(sum_buf, j)[...] + piece(mate_buf, j)[...]
                scaled = total * lax.rsqrt(jnp.mean(total * total, axis=-1, keepdims=True) + NORM_EPS)
                done = (piece(res_ref, j)[...].astype(jnp.float32) + scaled * gain_ref[...]).astype(jnp.bfloat16)
                piece(res_buf, j)[...] = done.astype(jnp.float32)
                piece(out_ref, j)[...] = done.astype(out_ref.dtype)
                copy(res_buf, res_buf, 2, j, outer).start()
        for c in range(chunks):
            copy(sum_buf, mate_buf, 1, c, mate).wait_send()
            copy(res_buf, res_buf, 2, c, outer).wait_send()


def line_reduce(part, residual, gain, out_dtype, collective_id, chunks=8, lag=2):
    rows, width = part.shape
    return pl.pallas_call(
        functools.partial(line_reduce_kernel, chunks, lag),
        out_shape=jax.ShapeDtypeStruct((rows, width), out_dtype),
        in_specs=[pl.BlockSpec(memory_space=pltpu.VMEM)] * 3,
        out_specs=pl.BlockSpec(memory_space=pltpu.VMEM),
        scratch_shapes=[pltpu.VMEM((rows, width), jnp.float32)] * 4 + [pltpu.SemaphoreType.DMA((3, chunks))] * 2,
        compiler_params=pltpu.CompilerParams(collective_id=collective_id, has_side_effects=True),
        cost_estimate=pl.CostEstimate(flops=60_000_000_000, bytes_accessed=4 * rows * width, transcendentals=0),
        name=f'line_reduce_{collective_id}',
    )(part, residual, 1.0 + gain.astype(jnp.float32)[None, :])


def head_kernel(tiles, y_in, gain_ref, tgt_ref, e_hbm, lp_ref, y_ref, e_buf, gath, h_buf, log_a, log_b, acc_s, acc_t,
                stat, plane_stat, part_stat, line_stat, e_sem, own_send, fwd_send, unit_recv, st_send, st_recv, ln_send, ln_recv):
    v = lax.axis_index('v')
    t = lax.axis_index('t')
    vy, vx, vc = v // 4, (v // 2) % 2, v % 2
    units, unit_rows, width = gath.shape
    row_tile = e_buf.shape[0] // tiles
    group = 4 * unit_rows

    def block(yf, xf, cf):
        return (vy + yf) % 2 * 4 + (vx + xf) % 2 * 2 + (vc + cf) % 2

    here, pair, near_x, near_y = block(0, 0, 0), block(0, 0, 1), block(0, 1, 0), block(1, 0, 0)

    def tile_copy(k):
        part = pl.ds(k * row_tile, row_tile)
        return pltpu.make_async_copy(e_hbm.at[part], e_buf.at[part], e_sem.at[k])

    def fetch(k, carry):
        tile_copy(k).start()
        return carry

    lax.fori_loop(0, tiles, fetch, 0)

    barrier = pltpu.get_barrier_semaphore()
    for d in range(1, 8):
        pl.semaphore_signal(barrier, inc=1, device_id={'v': (v + d) % 8}, device_id_type=MESH)
    for d in range(1, 4):
        pl.semaphore_signal(barrier, inc=1, device_id={'t': (t + d) % 4}, device_id_type=MESH)
    pl.semaphore_wait(barrier, 10)

    def own_copy(h, i, to):
        return pltpu.make_async_remote_copy(
            src_ref=y_in.at[h], dst_ref=gath.at[2 * here + h], send_sem=own_send.at[h, i],
            recv_sem=unit_recv.at[2 * here + h], device_id={'v': to}, device_id_type=MESH)

    def forward(u, i, to):
        return pltpu.make_async_remote_copy(
            src_ref=gath.at[u], dst_ref=gath.at[u], send_sem=fwd_send.at[i],
            recv_sem=unit_recv.at[u], device_id={'v': to}, device_id_type=MESH)

    def arrived(u):
        pltpu.make_async_remote_copy(
            src_ref=gath.at[u], dst_ref=gath.at[u], send_sem=fwd_send.at[0],
            recv_sem=unit_recv.at[u], device_id={'v': pair}, device_id_type=MESH).wait_recv()

    for h in range(2):
        own_copy(h, 0, near_x).start()
        own_copy(h, 1, near_y).start()
        own_copy(h, 2, pair).start()
    for h in range(2):
        gath[2 * here + h] = y_in[h]

    def unit_of(g, q):
        mid = jnp.logical_or(g == 1, g == 2)
        half = jnp.where(mid, g - 1, q % 2)
        xf = jnp.where(mid, 1 - q % 2, g // 3)
        yf = jnp.where(mid, q % 2, g // 3)
        return 2 * block(yf, xf, q // 2) + half

    def far(yf, xf, cf, h):
        return 2 * block(yf, xf, cf) + h

    first_row = (v * 4 + t) * e_buf.shape[0]
    sub_rows = row_tile // 10 if (row_tile // 10) % 8 == 0 else row_tile

    def group_step(g, carry):
        @pl.when(g == 0)
        def _():
            for h in range(2):
                arrived(far(0, 0, 1, h))

        for k in range(2):
            @pl.when(g == 1 + k)
            def _():
                ux, uy = far(0, 1, 0, k), far(1, 0, 0, k)
                arrived(ux)
                if k == 0:
                    forward(ux, 0, near_y).start()
                forward(ux, 2 + k, pair).start()
                arrived(uy)
                if k == 1:
                    forward(uy, 1, near_x).start()
                forward(uy, 4 + k, pair).start()
                arrived(far(0, 1, 1, k))
                arrived(far(1, 0, 1, k))

        @pl.when(g == 3)
        def _():
            for h in range(2):
                arrived(far(1, 1, 0, h))
                forward(far(1, 1, 0, h), 6 + h, pair).start()
            for h in range(2):
                arrived(far(1, 1, 1, h))

        lanes = []
        for q in range(4):
            u = unit_of(g, q)
            y = gath[u]
            y_ref[u] = y.astype(jnp.bfloat16)
            h = y * lax.rsqrt(jnp.mean(y * y, axis=-1, keepdims=True) + NORM_EPS) * gain_ref[...]
            h_buf[q * unit_rows:(q + 1) * unit_rows, :] = h.astype(jnp.bfloat16)
            lanes.append(tgt_ref[pl.ds(u, 1), :])
        local_tgt = jnp.concatenate(lanes, axis=1) - first_row
        acc_s[...] = jnp.zeros_like(acc_s)
        acc_t[...] = jnp.zeros_like(acc_t)

        def logits(r, dst):
            @pl.when(g == 0)
            def _():
                tile_copy(r).wait()
            start = pl.multiple_of(r * row_tile, row_tile)
            dst[...] = lax.dot_general(e_buf[pl.ds(start, row_tile), :], h_buf[...], (((1,), (1,)), ((), ())), preferred_element_type=jnp.float32)

        def reduce_tile(r, src):
            total_s, total_t = acc_s[...], acc_t[...]
            sub = lax.broadcasted_iota(jnp.int32, (sub_rows, group), 0)
            for p in range(row_tile // sub_rows):
                capped = jnp.tanh(src[p * sub_rows:(p + 1) * sub_rows, :] * (1.0 / FINAL_CAP))
                hit = sub == local_tgt - (r * row_tile + p * sub_rows)
                powers = jnp.exp2(capped * (FINAL_CAP * math.log2(math.e)))
                total_s = total_s + jnp.sum(powers.reshape(sub_rows // 8, 8, group), axis=0)
                total_t = total_t + jnp.sum(jnp.where(hit, capped, 0.0).reshape(sub_rows // 8, 8, group), axis=0)
            acc_s[...] = total_s
            acc_t[...] = total_t

        logits(0, log_a)

        def pair_step(i, c):
            logits(2 * i + 1, log_b)
            reduce_tile(2 * i, log_a)
            logits(2 * i + 2, log_a)
            reduce_tile(2 * i + 1, log_b)
            return c

        lax.fori_loop(0, tiles // 2 - 1, pair_step, 0)
        logits(tiles - 1, log_b)
        reduce_tile(tiles - 2, log_a)
        reduce_tile(tiles - 1, log_b)

        sums = jnp.sum(acc_s[...], axis=0, keepdims=True)
        hits = jnp.sum(acc_t[...], axis=0, keepdims=True) * FINAL_CAP
        for q in range(4):
            u = unit_of(g, q)
            stat[0, pl.ds(u, 1), :] = sums[:, q * unit_rows:(q + 1) * unit_rows]
            stat[1, pl.ds(u, 1), :] = hits[:, q * unit_rows:(q + 1) * unit_rows]
        return carry

    lax.fori_loop(0, 4, group_step, 0)

    def plane_copy(d):
        return pltpu.make_async_remote_copy(
            src_ref=stat, dst_ref=plane_stat.at[v], send_sem=st_send.at[d - 1],
            recv_sem=st_recv.at[v], device_id={'v': (v + d) % 8}, device_id_type=MESH)

    def plane_wait(d):
        other = (v + d) % 8
        pltpu.make_async_remote_copy(
            src_ref=stat, dst_ref=plane_stat.at[other], send_sem=st_send.at[d - 1],
            recv_sem=st_recv.at[other], device_id={'v': other}, device_id_type=MESH).wait_recv()

    def line_copy(d):
        return pltpu.make_async_remote_copy(
            src_ref=part_stat, dst_ref=line_stat.at[t], send_sem=ln_send.at[d - 1],
            recv_sem=ln_recv.at[t], device_id={'t': (t + d) % 4}, device_id_type=MESH)

    def line_wait(d):
        other = (t + d) % 4
        pltpu.make_async_remote_copy(
            src_ref=part_stat, dst_ref=line_stat.at[other], send_sem=ln_send.at[d - 1],
            recv_sem=ln_recv.at[other], device_id={'t': other}, device_id_type=MESH).wait_recv()

    for d in range(1, 8):
        plane_copy(d).start()
    plane_stat[v] = stat[...]
    for d in range(1, 8):
        plane_wait(d)
    part_stat[...] = jnp.sum(plane_stat[...], axis=0)
    for d in range(1, 4):
        line_copy(d).start()
    line_stat[t] = part_stat[...]
    for d in range(1, 4):
        line_wait(d)
    final = line_stat[0] + line_stat[1] + line_stat[2] + line_stat[3]
    lp_ref[...] = final[1] - jnp.log(final[0])

    for h in range(2):
        for i, to in enumerate((near_x, near_y, pair)):
            own_copy(h, i, to).wait_send()
    forward(far(0, 1, 0, 0), 0, near_y).wait_send()
    forward(far(1, 0, 0, 1), 1, near_x).wait_send()
    for k in range(2):
        forward(far(0, 1, 0, k), 2 + k, pair).wait_send()
        forward(far(1, 0, 0, k), 4 + k, pair).wait_send()
        forward(far(1, 1, 0, k), 6 + k, pair).wait_send()
    for d in range(1, 8):
        plane_copy(d).wait_send()
    for d in range(1, 4):
        line_copy(d).wait_send()


def gather_and_head(y_block, gain, target, embed_table, collective_id, tiles=10):
    rows, width = y_block.shape
    unit_rows = rows // 2
    vocab_local = embed_table.shape[0]
    row_tile = vocab_local // tiles
    dma = pltpu.SemaphoreType.DMA
    stat_shape = (2, 16, unit_rows)
    logprob, hidden_out = pl.pallas_call(
        functools.partial(head_kernel, tiles),
        out_shape=(jax.ShapeDtypeStruct((16, unit_rows), jnp.float32), jax.ShapeDtypeStruct((16, unit_rows, width), jnp.bfloat16)),
        in_specs=[pl.BlockSpec(memory_space=pltpu.VMEM)] * 3 + [pl.BlockSpec(memory_space=pl.ANY)],
        out_specs=(pl.BlockSpec(memory_space=pltpu.VMEM), pl.BlockSpec(memory_space=pltpu.VMEM)),
        scratch_shapes=[
            pltpu.VMEM((vocab_local, width), jnp.bfloat16),
            pltpu.VMEM((16, unit_rows, width), jnp.float32),
            pltpu.VMEM((4 * unit_rows, width), jnp.bfloat16),
            pltpu.VMEM((row_tile, 4 * unit_rows), jnp.float32),
            pltpu.VMEM((row_tile, 4 * unit_rows), jnp.float32),
            pltpu.VMEM((8, 4 * unit_rows), jnp.float32),
            pltpu.VMEM((8, 4 * unit_rows), jnp.float32),
            pltpu.VMEM(stat_shape, jnp.float32),
            pltpu.VMEM((8,) + stat_shape, jnp.float32),
            pltpu.VMEM(stat_shape, jnp.float32),
            pltpu.VMEM((4,) + stat_shape, jnp.float32),
            dma((tiles,)), dma((2, 3)), dma((8,)), dma((16,)), dma((7,)), dma((8,)), dma((3,)), dma((4,)),
        ],
        compiler_params=pltpu.CompilerParams(collective_id=collective_id, has_side_effects=True, vmem_limit_bytes=VMEM_LIMIT),
        cost_estimate=pl.CostEstimate(flops=2 * 8 * rows * width * vocab_local, bytes_accessed=2 * vocab_local * width, transcendentals=2 * 8 * rows * vocab_local),
        name='gather_and_head',
    )(y_block.reshape(2, unit_rows, width), 1.0 + gain.astype(jnp.float32)[None, :], target.reshape(16, unit_rows), embed_table)
    return logprob.reshape(8 * rows), hidden_out.reshape(8 * rows, width)


def solution(mesh):
    v_size = mesh.shape['v']
    in_specs = (P(), P(), P(), P(), P(None, 't'), P(None, 't'), P(None, 't'), P('t', None), P(), P(), P(None, 't'), P(None, 't'), P('t', None), P(), P(), P(None, None, 't', None), P(None, None, 't', None), P(('v', 't'), None))

    def local_step(hidden_in, seq_lens, target, g_attn_pre, w_q, w_k, w_v, w_o, g_attn_post, g_mlp_pre, w_gate, w_up, w_down, g_mlp_post, g_final, k_cache, v_cache, embed_table):
        rows = hidden_in.shape[0] // v_size
        start = lax.axis_index('v') * rows

        def mine(array):
            return lax.dynamic_slice_in_dim(array, start, rows, 0)

        x, lens = mine(hidden_in), mine(seq_lens)
        normed = rms_norm(x, g_attn_pre).astype(jnp.bfloat16)
        attn_vec = attention(normed, lens, w_q, w_k, w_v, mine(k_cache), mine(v_cache))
        attn_part = jnp.dot(attn_vec, w_o, preferred_element_type=jnp.float32)
        hidden_mid = line_reduce(attn_part, x, g_attn_post, jnp.bfloat16, 0)
        mlp_in = rms_norm(hidden_mid, g_mlp_pre).astype(jnp.bfloat16)
        gate_proj = jnp.dot(mlp_in, w_gate, preferred_element_type=jnp.float32)
        up_proj = jnp.dot(mlp_in, w_up, preferred_element_type=jnp.float32)
        activated = (jax.nn.gelu(gate_proj, approximate=True) * up_proj).astype(jnp.bfloat16)
        mlp_part = jnp.dot(activated, w_down, preferred_element_type=jnp.float32)
        y_block = line_reduce(mlp_part, hidden_mid, g_mlp_post, jnp.float32, 1)
        return gather_and_head(y_block, g_final, target, embed_table, 2)

    return jax.shard_map(local_step, mesh=mesh, in_specs=in_specs, out_specs=(P(), P()), check_vma=False)
```
